8 devices in a mesh: stage: 1 (over z), x2: 2 (over y), y: 2 (over x), x: 2 (over core).
Axes of the slice: x: 2, y: 2, z: 1, core: 2. Of those that a mesh axis runs over, the one named last changes fastest.
Arguments:
- mu: float32 [], replicated
- eta: float32 [], replicated
- x_wq: float32 [2048, 2048], P(('stage', 'x2', 'x'), 'y')
- m_wq: float32 [2048, 2048], P(('stage', 'x2', 'x'), 'y')
- g_wq: bfloat16 [2048, 2048], P(('stage', 'x2', 'x'), 'y')
- f_wq: float32 [2048, 64], P(('stage', 'y'))
- x_wk: float32 [2048, 512], P(('stage', 'x2', 'x'), 'y')
- m_wk: float32 [2048, 512], P(('stage', 'x2', 'x'), 'y')
- g_wk: bfloat16 [2048, 512], P(('stage', 'x2', 'x'), 'y')
- f_wk: float32 [512, 16], P(('stage', 'y'))
- x_wv: float32 [2048, 512], P(('stage', 'x2', 'x'), 'y')
- m_wv: float32 [2048, 512], P(('stage', 'x2', 'x'), 'y')
- g_wv: bfloat16 [2048, 512], P(('stage', 'x2', 'x'), 'y')
- f_wv: float32 [512, 16], P(('stage', 'y'))
- x_wo: float32 [2048, 2048], P(('stage', 'x2', 'x'), 'y')
- m_wo: float32 [2048, 2048], P(('stage', 'x2', 'x'), 'y')
- g_wo: bfloat16 [2048, 2048], P(('stage', 'x2', 'x'), 'y')
- f_wo: float32 [2048, 64], P(('stage', 'y'))
- x_wg: float32 [2048, 8192], P(('stage', 'x2', 'x'), 'y')
- m_wg: float32 [2048, 8192], P(('stage', 'x2', 'x'), 'y')
- g_wg: bfloat16 [2048, 8192], P(('stage', 'x2', 'x'), 'y')
- f_wg: float32 [2048, 64], P(('stage', 'x2', 'x'))
- x_wu: float32 [2048, 8192], P(('stage', 'x2', 'x'), 'y')
- m_wu: float32 [2048, 8192], P(('stage', 'x2', 'x'), 'y')
- g_wu: bfloat16 [2048, 8192], P(('stage', 'x2', 'x'), 'y')
- f_wu: float32 [2048, 64], P(('stage', 'x2', 'x'))
- x_wd: float32 [8192, 2048], P(('stage', 'x2', 'x'), 'y')
- m_wd: float32 [8192, 2048], P(('stage', 'x2', 'x'), 'y')
- g_wd: bfloat16 [8192, 2048], P(('stage', 'x2', 'x'), 'y')
- f_wd: float32 [2048, 64], P(('stage', 'y'))
Outputs:
- output 1: float32 [2048, 2048], P(('stage', 'x2', 'x'), 'y')
- output 2: float32 [2048, 2048], P(('stage', 'x2', 'x'), 'y')
- output 3: float32 [2048, 64], P(('stage', 'y'))
- output 4: float32 [2048, 512], P(('stage', 'x2', 'x'), 'y')
- output 5: float32 [2048, 512], P(('stage', 'x2', 'x'), 'y')
- output 6: float32 [512, 16], P(('stage', 'y'))
- output 7: float32 [2048, 512], P(('stage', 'x2', 'x'), 'y')
- output 8: float32 [2048, 512], P(('stage', 'x2', 'x'), 'y')
- output 9: float32 [512, 16], P(('stage', 'y'))
- output 10: float32 [2048, 2048], P(('stage', 'x2', 'x'), 'y')
- output 11: float32 [2048, 2048], P(('stage', 'x2', 'x'), 'y')
- output 12: float32 [2048, 64], P(('stage', 'y'))
- output 13: float32 [2048, 8192], P(('stage', 'x2', 'x'), 'y')
- output 14: float32 [2048, 8192], P(('stage', 'x2', 'x'), 'y')
- output 15: float32 [2048, 64], P(('stage', 'x2', 'x'))
- output 16: float32 [2048, 8192], P(('stage', 'x2', 'x'), 'y')
- output 17: float32 [2048, 8192], P(('stage', 'x2', 'x'), 'y')
- output 18: float32 [2048, 64], P(('stage', 'x2', 'x'))
- output 19: float32 [8192, 2048], P(('stage', 'x2', 'x'), 'y')
- output 20: float32 [8192, 2048], P(('stage', 'x2', 'x'), 'y')
- output 21: float32 [2048, 64], P(('stage', 'y'))
All inputs are finite; a program needn't handle non-finite values.
Results may differ from the reference program's by a relative error of at most 0.001.
Values are sent between devices in bfloat16 or wider.
A program may use at most 1 GiB of HBM per device.

```python
import math
import jax
import jax.numpy as jnp
from jax import lax

D = 2048
FFN = 8192
KV_HEADS = 8
HEAD = 64
RDIV = 32

KVW = KV_HEADS * HEAD
HI = lax.Precision.HIGHEST
MATS = (('wq', D, D, False), ('wk', D, KVW, False), ('wv', D, KVW, False), ('wo', D, D, False), ('wg', D, FFN, True), ('wu', D, FFN, True), ('wd', FFN, D, False))


def profile(key, length):
    k1, k2 = jax.random.split(key)
    phase = jax.random.uniform(k1, (), jnp.float32, 0.0, 6.2832)
    t = jnp.arange(length, dtype=jnp.float32) / length
    wob = jax.random.uniform(k2, (length,), jnp.float32, -0.15, 0.15)
    return jnp.exp(0.3 * jnp.sin(6.2832 * t + phase)) * (1.0 + wob)


def setup_inputs(seed: int = 0, part: int = 0) -> dict:
    key = jax.random.key(seed)
    kmu, keta = jax.random.split(jax.random.fold_in(key, 1000003))
    kpart = jax.random.fold_in(key, part)
    out = {}
    out['mu'] = jax.random.uniform(kmu, (), jnp.float32, 0.8, 0.95)
    out['eta'] = jax.random.uniform(keta, (), jnp.float32, 0.15, 0.25) * ((D * KVW) ** 0.25) * (RDIV ** 0.5)
    for i, mat in enumerate(MATS):
        name, rows, cols = mat[0], mat[1], mat[2]
        ks = jax.random.split(jax.random.fold_in(kpart, i), 8)
        n = min(rows, cols)
        r = n // RDIV
        k = 2 * r
        sc = profile(ks[0], rows)[:, None] * profile(ks[1], cols)[None, :]
        u = jax.random.normal(ks[2], (rows, k), jnp.float32)
        v = jax.random.normal(ks[3], (cols, k), jnp.float32)
        low = jnp.dot(u, v.T) * (k ** -0.5)
        noise = jax.random.normal(ks[4], (rows, cols), jnp.float32)
        out['x_' + name] = jax.random.normal(ks[5], (rows, cols), jnp.float32)
        out['m_' + name] = 0.8 * jax.random.normal(ks[6], (rows, cols), jnp.float32) * sc
        out['g_' + name] = ((low + 0.5 * noise) * sc).astype(jnp.bfloat16)
        out['f_' + name] = jax.random.normal(ks[7], (n, r), jnp.float32) * (n ** -0.5)
    return out


def dion_one(x, mo, g, f, mu, eta, tr):
    b = mo + g.astype(jnp.float32)
    if tr:
        b = b.T
        x = x.T
    pt = jnp.dot(b, f, precision=HI, preferred_element_type=jnp.float32)
    w = jnp.dot(pt.T, pt, precision=HI, preferred_element_type=jnp.float32)
    lo = jnp.linalg.cholesky(w)
    p = lax.linalg.triangular_solve(lo, pt, left_side=False, lower=True, transpose_a=True)
    rr = jnp.dot(b.T, p, precision=HI, preferred_element_type=jnp.float32)
    m_new = b - (1.0 - mu) * jnp.dot(p, rr.T, precision=HI, preferred_element_type=jnp.float32)
    f_new = rr / jnp.sqrt(jnp.sum(rr * rr, axis=0))
    x_new = x - (eta * math.sqrt(b.shape[0] / b.shape[1])) * jnp.dot(p, f_new.T, precision=HI, preferred_element_type=jnp.float32)
    if tr:
        return x_new.T, m_new.T, f_new
    return x_new, m_new, f_new


def reference(mu, eta, x_wq, m_wq, g_wq, f_wq, x_wk, m_wk, g_wk, f_wk, x_wv, m_wv, g_wv, f_wv, x_wo, m_wo, g_wo, f_wo, x_wg, m_wg, g_wg, f_wg, x_wu, m_wu, g_wu, f_wu, x_wd, m_wd, g_wd, f_wd):
    xn_q, mn_q, fn_q = dion_one(x_wq, m_wq, g_wq, f_wq, mu, eta, False)
    xn_k, mn_k, fn_k = dion_one(x_wk, m_wk, g_wk, f_wk, mu, eta, False)
    xn_v, mn_v, fn_v = dion_one(x_wv, m_wv, g_wv, f_wv, mu, eta, False)
    xn_o, mn_o, fn_o = dion_one(x_wo, m_wo, g_wo, f_wo, mu, eta, False)
    xn_g, mn_g, fn_g = dion_one(x_wg, m_wg, g_wg, f_wg, mu, eta, True)
    xn_u, mn_u, fn_u = dion_one(x_wu, m_wu, g_wu, f_wu, mu, eta, True)
    xn_d, mn_d, fn_d = dion_one(x_wd, m_wd, g_wd, f_wd, mu, eta, False)
    return (xn_q, mn_q, fn_q, xn_k, mn_k, fn_k, xn_v, mn_v, fn_v, xn_o, mn_o, fn_o, xn_g, mn_g, fn_g, xn_u, mn_u, fn_u, xn_d, mn_d, fn_d)
```

```python
import math
import jax
import jax.numpy as jnp
from jax import lax
from jax.experimental import pallas as pl
from jax.experimental.pallas import tpu as pltpu
from jax.sharding import PartitionSpec as P

F32 = jnp.float32
BF16 = jnp.bfloat16
HI = lax.Precision.HIGHEST
ROWS = ('stage', 'x2', 'x')
TRANS = (False, False, False, False, True, True, False)
VLIM = 28 * 1024 * 1024
LN = 128

VM = pl.BlockSpec(memory_space=pltpu.VMEM)
SM = pl.BlockSpec(memory_space=pltpu.SMEM)
HB = pl.BlockSpec(memory_space=pltpu.HBM)


def _dot(a, b, ca, cb, prec=None):
    return lax.dot_general(a, b, (((ca,), (cb,)), ((), ())), precision=prec, preferred_element_type=F32)


def nn(a, b):
    return _dot(a, b, 1, 0)


def nt(a, b):
    return _dot(a, b, 1, 1)


def split3(x):
    a = x.astype(BF16)
    r = x - a.astype(F32)
    b = r.astype(BF16)
    return a, b, (r - b.astype(F32)).astype(BF16)


def fsplit(x):
    return [t.astype(F32) for t in split3(x)]


def rhs_cat(t):
    r = t.shape[0]
    a, b, c = split3(t)
    parts = [a, b, a, c, b, a]
    if r * 6 < LN:
        parts.append(jnp.zeros((LN - 6 * r, t.shape[1]), BF16))
    return jnp.concatenate(parts, 0)


def lhs_cat(t):
    r, m = t.shape
    reps = LN // r
    w = jnp.concatenate([t] * reps, 0).T
    a, b, c = split3(w)
    grp = lax.broadcasted_iota(jnp.int32, (m, LN), 1) // r
    if reps == 2:
        lo = grp == 0
        a, b, c = a.astype(F32), b.astype(F32), c.astype(F32)
        return jnp.concatenate([a, jnp.where(lo, b, a), jnp.where(lo, b, c)], 1).astype(BF16)
    a, b, c = a.astype(F32), b.astype(F32), c.astype(F32)
    z = jnp.where(grp < 2, a, jnp.where(grp == 2, b, jnp.where(grp == 3, a, jnp.where(grp == 4, b, c))))
    return jnp.where(grp < 6, z, 0.0).astype(BF16)


def stack_k(t, width):
    a, b, c = fsplit(t)
    k, r = t.shape
    z = lambda n: jnp.zeros((k, n), F32)
    x0 = jnp.concatenate([a, b, c, z(width - 3 * r)], 1)
    x1 = jnp.concatenate([a, b, z(width - 2 * r)], 1)
    x2 = jnp.concatenate([a, z(width - r)], 1)
    return jnp.concatenate([x0, x1, x2], 0).astype(BF16)


def fold_t(acc, r):
    if acc.shape[1] == 2 * LN:
        acc = acc[:, :LN] + acc[:, LN:]
    t = acc.T
    if r == LN // 2:
        return t[:r] + t[r:]
    return t[:r] + (t[r:2 * r] + t[2 * r:3 * r])


def left_prod(pc, b, r):
    b0, b1, b2 = split3(b)
    a0, a1, a2 = nn(pc, b0), nn(pc[:2 * r], b1), nn(pc[:r], b2)
    return a0[:r] + ((a0[r:2 * r] + a1[:r]) + ((a0[2 * r:] + a1[r:]) + a2))


def gram(p):
    r = p.shape[0]
    z = [jnp.zeros((64, p.shape[1]), F32), p]
    if r < 64:
        z.append(jnp.zeros((64 - r, p.shape[1]), F32))
    return _dot(p, jnp.concatenate(z, 0), 1, 1, HI)


def chol_inv(ws):
    mats = []
    for w in ws:
        r = w.shape[0]
        ri = lax.broadcasted_iota(jnp.int32, (r, LN), 0)
        li = lax.broadcasted_iota(jnp.int32, (r, LN), 1)
        a = jnp.where(li < 64, jnp.where(ri == li, 1.0, 0.0), w)
        mats.append([a[8 * k:8 * k + 8] for k in range(r // 8)])
    sub = lax.broadcasted_iota(jnp.int32, (8, LN), 0)
    for j in range(max(8 * len(g) for g in mats)):
        k0, s = j // 8, j % 8
        for g in mats:
            if j >= 8 * len(g):
                continue
            row = g[k0][s:s + 1, :]
            d = row[:, 64 + j:65 + j]
            rs = lax.rsqrt(d)
            rs = rs * (1.5 - 0.5 * ((d * rs) * rs))
            row = row * rs
            for k in range(k0, len(g)):
                col = g[k][:, 64 + j:65 + j] * rs
                upd = g[k] - col * row
                if k == k0:
                    upd = jnp.where(sub > s, upd, jnp.where(sub == s, row, g[k]))
                g[k] = upd
    return [jnp.concatenate(g, 0) for g in mats]


def ka_t(core, m, g, f, b, keep, send, fc, *, ct):
    rows, cols = m.shape
    r = f.shape[1]
    nb = cols // ct
    half = nb // 2
    fc[...] = jnp.concatenate(split3(f[...].T), 0)

    def body(mb, gb):
        i = pl.program_id(0)
        bb = mb[...] + gb[...].astype(F32)
        b[:, pl.ds(pl.multiple_of(i * ct, ct), ct)] = bb
        p = left_prod(fc[...], bb, r)
        mine = (i // half) == core[0]
        at = pl.ds(pl.multiple_of((i % half) * ct, ct), ct)

        @pl.when(mine)
        def _():
            keep[:, at] = p

        @pl.when(jnp.logical_not(mine))
        def _():
            send[:, at] = p

    spec = pl.BlockSpec((rows, ct), lambda i: (0, i))
    pltpu.emit_pipeline(body, grid=(nb,), in_specs=[spec, spec])(m, g)


def ka_n(*refs, rt, k):
    ms, gs, fs = refs[:k], refs[k:2 * k], refs[2 * k:3 * k]
    bs, pt = refs[3 * k:4 * k], refs[4 * k]
    fcs = refs[4 * k + 1:]
    rows = ms[0].shape[0]
    for f, fc in zip(fs, fcs):
        fc[...] = stack_k(f[...], fc.shape[1])

    def body(*blk):
        i = pl.program_id(0)
        at = pl.ds(pl.multiple_of(i * rt, rt), rt)
        o = 0
        for mb, gb, b, f, fc in zip(blk[:k], blk[k:], bs, fs, fcs):
            r = f.shape[1]
            bb = mb[...] + gb[...].astype(F32)
            b[at, :] = bb
            acc = nn(jnp.concatenate(split3(bb), 1), fc[...])
            pt[o:o + r, at] = fold_t(acc, r)
            o += r

    specs = [pl.BlockSpec((rt, m.shape[1]), lambda i: (i, 0)) for m in ms]
    pltpu.emit_pipeline(body, grid=(rows // rt,), in_specs=specs + specs)(*ms, *gs)


def kz_t(core, b, hs, other, pt, zw, acc, *, ct):
    rows, cols = b.shape
    r = hs.shape[0]
    half = cols // 2
    c = core[0]
    pt[:, pl.ds(pl.multiple_of(c * half, half), half)] = hs[...]
    pt[:, pl.ds(pl.multiple_of((1 - c) * half, half), half)] = other[...]
    acc[...] = jnp.zeros_like(acc)

    def step(i, _):
        at = pl.ds(pl.multiple_of(i * ct, ct), ct)
        p0, p1, p2 = split3(pt[:, at])
        z = jnp.zeros((r, ct), BF16)
        w = jnp.concatenate([jnp.concatenate([p0, p1, p2, z], 0), jnp.concatenate([p0, p1, z, z], 0), jnp.concatenate([p0, z, z, z], 0)], 1)
        acc[...] += nt(jnp.concatenate(split3(b[:, at]), 1), w)
        return 0

    lax.fori_loop(0, cols // ct, step, 0)
    zw[:, :rows] = fold_t(acc[...], r)
    zw[:, rows:] = gram(pt[...])


def _zn(b, p, r, ct):
    rows, cols = b.shape
    pc = jnp.concatenate(split3(p), 0)
    out = []
    for c0 in range(0, cols, ct):
        z = None
        for r0 in range(0, rows, 512):
            t = left_prod(pc[:, r0:r0 + 512], b[r0:r0 + 512, c0:c0 + ct], r)
            z = t if z is None else z + t
        out.append(z)
    return out


def kz_d(core, b, own, rec, pt, keep, send, zs):
    p = own[...] + rec[...]
    pt[...] = p
    r, cols = p.shape[0], b.shape[1]
    half = cols // 2
    w = gram(p)
    keep[:, half:] = w
    send[:, half:] = w
    for n, z in enumerate(_zn(b, p, r, 256)):
        zs[:, n * 256:(n + 1) * 256] = z
    c = core[0]
    keep[:, :half] = zs[:, pl.ds(pl.multiple_of(c * half, half), half)]
    send[:, :half] = zs[:, pl.ds(pl.multiple_of((1 - c) * half, half), half)]


def kz_a(core, bq, bo, bk, bv, own, rec, pt, keep, send, zq, zk):
    p = own[...] + rec[...]
    pt[...] = p
    c = core[0]
    nq, nk = bq.shape[1], bk.shape[1]
    hq, hk = nq // 2, nk // 2
    for n, b in enumerate((bq, bo)):
        q = p[64 * n:64 * n + 64]
        w = gram(q)
        at = slice(2 * hq + n * LN, 2 * hq + (n + 1) * LN)
        keep[:, at] = w
        send[:, at] = w
        for i, z in enumerate(_zn(b, q, 64, 256)):
            zq[n, :, i * 256:(i + 1) * 256] = z
        keep[:, n * hq:(n + 1) * hq] = zq[n, :, pl.ds(pl.multiple_of(c * hq, hq), hq)]
        send[:, n * hq:(n + 1) * hq] = zq[n, :, pl.ds(pl.multiple_of((1 - c) * hq, hq), hq)]
    at = slice(2 * hq + 2 * LN, 2 * hq + 3 * LN)
    for n, b in enumerate((bk, bv)):
        q = p[128 + 16 * n:144 + 16 * n]
        w = gram(q)
        keep[32 + 16 * n:48 + 16 * n, at] = w
        send[32 + 16 * n:48 + 16 * n, at] = w
        zk[n] = _zn(b, q, 16, 256)[0]
        keep[16 * n:16 * n + 16, at] = zk[n, :, pl.ds(pl.multiple_of(c * hk, hk), hk)]
        send[16 * n:16 * n + 16, at] = zk[n, :, pl.ds(pl.multiple_of((1 - c) * hk, hk), hk)]


def _rn(lin, zt):
    rt = _dot(lin[:, :lin.shape[0]], zt, 1, 0, HI)
    s = jnp.sum(rt * rt, axis=1, keepdims=True)
    return rt, jnp.broadcast_to(s, (rt.shape[0], LN))


def kc_t(own0, rec0, own1, rec1, rt0, rt1, lin0, lin1, ss):
    n = rt0.shape[1]
    z = [own0[...] + rec0[...], own1[...] + rec1[...]]
    li = chol_inv([t[:, n:] for t in z])
    for i, (rt, lin) in enumerate(((rt0, lin0), (rt1, lin1))):
        lin[...] = li[i]
        rt[...], ss[64 * i:64 * i + 64] = _rn(li[i], z[i][:, :n])


def kc_n(core, ha, oa, hd, od, rq, ro, rk, rv, rd, lq, lo, lk, lv, ld, ss):
    c = core[0]
    nq = rq.shape[1]
    hq = nq // 2
    tq, tk = 2 * hq, 2 * hq + 2 * LN
    ws = [ha[:, tq:tq + LN], ha[:, tq + LN:tq + 2 * LN], ha[32:48, tk:], ha[48:64, tk:], hd[:, hd.shape[1] - LN:]]
    li = chol_inv(ws)
    rs = (rq, ro, rk, rv, rd)
    for i, (lin, rr) in enumerate(zip((lq, lo, lk, lv, ld), rs)):
        lin[...] = li[i]
        hn = rr.shape[1] // 2
        for src, at in ((0, c), (1, 1 - c)):
            a, d = (ha, hd) if src == 0 else (oa, od)
            if i < 2:
                z = a[:, i * hq:(i + 1) * hq]
            elif i < 4:
                z = a[16 * (i - 2):16 * (i - 2) + 16, tk:]
            else:
                z = d[:, :hn]
            rr[:, pl.ds(pl.multiple_of(at * hn, hn), hn)] = _dot(li[i][:, :rr.shape[0]], z, 1, 0, HI)
    o = 0
    for rr in rs:
        v = rr[...]
        r = v.shape[0]
        ss[o:o + r] = jnp.broadcast_to(jnp.sum(v * v, axis=1, keepdims=True), (r, LN))
        o += r


def _factors(rt, lin, ss, mu, eta, ratio, fo):
    r = rt.shape[0]
    li = lin[:, :r]
    v = rt[...]
    fn = v / jnp.sqrt(ss[:, :1])
    fo[...] = fn.T
    g1 = (1.0 - mu) * _dot(li, v, 0, 0, HI)
    g2 = (eta * ratio) * _dot(li, fn, 0, 0, HI)
    return g1, g2


def kf_t(mu, eta, b, x, pt, rt, lin, s0, s1, s2, s3, xo, mo, fo, c1, c2, *, ct, ratio, off):
    rows, cols = b.shape
    ss = (s0[off:off + 64] + s1[off:off + 64]) + (s2[off:off + 64] + s3[off:off + 64])
    g1, g2 = _factors(rt, lin, ss, mu[0], eta[0], ratio, fo)
    c1[...] = lhs_cat(g1)
    c2[...] = lhs_cat(g2)

    def body(xb, xob, mob):
        i = pl.program_id(0)
        at = pl.ds(pl.multiple_of(i * ct, ct), ct)
        w = rhs_cat(pt[:, at])
        mob[...] = b[:, at] - nn(c1[...], w)
        xob[...] = xb[...] - nn(c2[...], w)

    spec = pl.BlockSpec((rows, ct), lambda i: (0, i))
    pltpu.emit_pipeline(body, grid=(cols // ct,), in_specs=[spec], out_specs=[spec, spec])(x, xo, mo)


def kf_n(*refs, k, rt, ratios, offs):
    mu, eta = refs[:2]
    bs, xs, rts, lins = (refs[2 + i * k:2 + (i + 1) * k] for i in range(4))
    pt, s0, s1 = refs[2 + 4 * k:5 + 4 * k]
    rest = refs[5 + 4 * k:]
    xos, mos, fos = (rest[i * k:(i + 1) * k] for i in range(3))
    scr = rest[3 * k:]
    pcs, c1s, c2s = (scr[i * k:(i + 1) * k] for i in range(3))
    o = 0
    for i in range(k):
        r = rts[i].shape[0]
        so = offs[i]
        g1, g2 = _factors(rts[i], lins[i], s0[so:so + r] + s1[so:so + r], mu[0], eta[0], ratios[i], fos[i])
        c1s[i][...] = rhs_cat(g1)
        c2s[i][...] = rhs_cat(g2)
        pcs[i][...] = lhs_cat(pt[o:o + r])
        o += r

    def body(*blk):
        i = pl.program_id(0)
        at = pl.ds(pl.multiple_of(i * rt, rt), rt)
        for n in range(k):
            pc = pcs[n][at, :]
            blk[2 * k + n][...] = bs[n][at, :] - nn(pc, c1s[n][...])
            blk[k + n][...] = blk[n][...] - nn(pc, c2s[n][...])

    rows = bs[0].shape[0]
    specs = [pl.BlockSpec((rt, b.shape[1]), lambda i: (i, 0)) for b in bs]
    pltpu.emit_pipeline(body, grid=(rows // rt,), in_specs=specs, out_specs=specs + specs)(*xs, *xos, *mos)


def call(fn, ins, in_specs, outs, scratch, name, flops, nbytes):
    shapes, specs = [], []
    for kind, shape in outs:
        if kind == 'v':
            shapes.append(pltpu.VMEM(shape, F32))
            specs.append(VM)
        elif kind == 'h':
            shapes.append(jax.ShapeDtypeStruct(shape, F32))
            specs.append(HB)
        else:
            shapes.append(jax.ShapeDtypeStruct(shape, F32))
            specs.append(VM)
    return pl.pallas_call(
        fn, out_shape=tuple(shapes), in_specs=in_specs, out_specs=tuple(specs), scratch_shapes=scratch, name=name,
        compiler_params=pltpu.CompilerParams(vmem_limit_bytes=VLIM),
        cost_estimate=pl.CostEstimate(flops=int(flops), bytes_accessed=int(nbytes), transcendentals=0))(*ins)


def swap(v, ax):
    return lax.ppermute(v, ax, [(0, 1), (1, 0)])


def local(mu, eta, *mats):
    mu, eta = mu.reshape(1), eta.reshape(1)
    core = lax.axis_index('x').astype(jnp.int32).reshape(1)
    x, m, g, f = (mats[i::4] for i in range(4))
    IQ, IK, IV, IO, IG, IU, ID = range(7)

    def cost(ids, passes, bpe):
        n = sum(m[i].size for i in ids)
        return n * 2 * 256 * passes, n * bpe

    def bsh(i):
        return ('v', m[i].shape)

    tr = {}
    for i in (IG, IU):
        rows, cols = m[i].shape
        r = f[i].shape[1]
        b, keep, send = call(
            lambda *a: ka_t(*a, ct=512), (core, m[i], g[i], f[i]), [SM, HB, HB, VM],
            [bsh(i), ('o', (r, cols // 2)), ('o', (r, cols // 2))], [pltpu.VMEM((3 * r, rows), BF16)], 'ka_t', *cost([i], 3, 6))
        tr[i] = [b, keep, swap(send, 'x')]
    for i in (IG, IU):
        tr[i].append(swap(tr[i][1] + tr[i][2], 'x2'))

    def an(ids, rt):
        k = len(ids)
        rows = m[ids[0]].shape[0]
        scr = [pltpu.VMEM((3 * m[i].shape[1], 256 if f[i].shape[1] == 64 else LN), BF16) for i in ids]
        res = call(
            lambda *a: ka_n(*a, rt=rt, k=k), [m[i] for i in ids] + [g[i] for i in ids] + [f[i] for i in ids],
            [HB] * (2 * k) + [VM] * k, [bsh(i) for i in ids] + [('o', (sum(f[i].shape[1] for i in ids), rows))], scr, 'ka_n', *cost(ids, 3, 6))
        return res[:k], res[k], swap(res[k], 'y')

    IA = (IQ, IO, IK, IV)
    ba, pa, qa = an(IA, 128)
    bd, pd, qd = an((ID,), 256)

    nq, nk, nd = m[IQ].shape[1], m[IK].shape[1], m[ID].shape[1]
    wa = nq + 3 * LN
    pta, keep_a, send_a = call(
        kz_a, (core, *ba, pa, qa), [SM] + [VM] * 6, [('o', pa.shape), ('o', (64, wa)), ('o', (64, wa))],
        [pltpu.VMEM((2, 64, nq), F32), pltpu.VMEM((2, 16, nk), F32)], 'kz_a', *cost(IA, 2, 0.1))
    ra = swap(send_a, 'x')
    wd = nd // 2 + LN
    ptd, keep_d, send_d = call(
        kz_d, (core, bd[0], pd, qd), [SM, VM, VM, VM], [('o', pd.shape), ('o', (64, wd)), ('o', (64, wd))],
        [pltpu.VMEM((64, nd), F32)], 'kz_d', *cost([ID], 2, 0.1))
    rd = swap(send_d, 'x')
    ha = keep_a + ra
    hd = keep_d + rd
    ha2 = swap(ha, 'x2')
    hd2 = swap(hd, 'x2')

    zt = {}
    for i in (IG, IU):
        b, keep, rec, rec2 = tr[i]
        hs = (keep + rec) + rec2
        other = swap(hs, 'x')
        rows, cols = b.shape
        r = hs.shape[0]
        pt, zw = call(
            lambda *a: kz_t(*a, ct=512), (core, b, hs, other), [SM, VM, VM, VM],
            [('o', (r, cols)), ('o', (r, rows + LN))], [pltpu.VMEM((rows, 256), F32)], 'kz_t', *cost([i], 3, 0.1))
        zt[i] = (pt, zw, swap(zw, 'y'))

    fa, fd = ha + ha2, hd + hd2
    oa, od = swap(fa, 'x'), swap(fd, 'x')
    rs = [('o', (f[i].shape[1], m[i].shape[1])) for i in (IQ, IO, IK, IV, ID)]
    ls = [('o', (f[i].shape[1], LN)) for i in (IQ, IO, IK, IV, ID)]
    res = call(kc_n, (core, fa, oa, fd, od), [SM] + [VM] * 4, rs + ls + [('o', (224, LN))], [], 'kc_n', 1e9, 1e7)
    rn, ln, ssn = res[:5], res[5:10], res[10]
    ssn2 = swap(ssn, 'y')

    nt_ = m[IG].shape[0]
    rt0, rt1, lin0, lin1, sst = call(
        kc_t, (zt[IG][1], zt[IG][2], zt[IU][1], zt[IU][2]), [VM] * 4,
        [('o', (64, nt_))] * 2 + [('o', (64, LN))] * 2 + [('o', (128, LN))], [], 'kc_t', 1e9, 1e7)
    sst1, sst2 = swap(sst, 'x'), swap(sst, 'x2')
    sst3 = lax.ppermute(sst, ('x2', 'x'), [(0, 3), (1, 2), (2, 1), (3, 0)])

    out = {}

    def fin_n(ids, bs, pt, sel, rt, offs):
        k = len(ids)
        ratios = [2.0 if i in (IK, IV, ID) else 1.0 for i in ids]
        kk = [384 if f[i].shape[1] == 64 else LN for i in ids]
        scr = [pltpu.VMEM((m[i].shape[0], q), BF16) for i, q in zip(ids, kk)]
        scr += [pltpu.VMEM((q, m[i].shape[1]), BF16) for i, q in zip(ids, kk)] * 2
        res = call(
            lambda *a: kf_n(*a, k=k, rt=rt, ratios=ratios, offs=offs),
            (mu, eta, *bs, *[x[i] for i in ids], *[rn[j] for j in sel], *[ln[j] for j in sel], pt, ssn, ssn2),
            [SM, SM] + [VM] * k + [HB] * k + [VM] * (2 * k + 3),
            [('h', m[i].shape) for i in ids] * 2 + [('o', f[i].shape) for i in ids], scr, 'kf_n', *cost(ids, 4, 12))
        for n, i in enumerate(ids):
            out[i] = (res[n], res[k + n], res[2 * k + n])

    fin_n(IA, ba, pta, (0, 1, 2, 3), 128, (0, 64, 128, 144))
    fin_n((ID,), bd, ptd, (4,), 256, (160,))
    for i, rt, lin, off in ((IG, rt0, lin0, 0), (IU, rt1, lin1, 64)):
        rows = m[i].shape[0]
        out[i] = call(
            lambda *a, off=off: kf_t(*a, ct=512, ratio=2.0, off=off),
            (mu, eta, tr[i][0], x[i], zt[i][0], rt, lin, sst, sst1, sst2, sst3), [SM, SM, VM, HB] + [VM] * 7,
            [('h', m[i].shape)] * 2 + [('o', f[i].shape)], [pltpu.VMEM((rows, 384), BF16)] * 2, 'kf_t', *cost([i], 4, 12))
    return tuple(v for i in range(7) for v in out[i])


def solution(mesh):
    spec_w = P(ROWS, 'y')
    spec_fy = P(('stage', 'y'), None)
    spec_ff = P(ROWS, None)
    in_specs = [P(), P()]
    out_specs = []
    for k in range(7):
        spec_f = spec_ff if TRANS[k] else spec_fy
        in_specs.extend([spec_w, spec_w, spec_w, spec_f])
        out_specs.extend([spec_w, spec_w, spec_f])
    return jax.shard_map(local, mesh=mesh, in_specs=tuple(in_specs), out_specs=tuple(out_specs), check_vma=False)
```
